32 devices in a mesh: dp: 2 (over x), tp: 16 (over z, y, core).
Axes of the slice: x: 2, y: 2, z: 4, core: 2. Of those that a mesh axis runs over, the one named last changes fastest.
Arguments:
- hidden: bfloat16 [128, 5, 4096], P('dp'), parts along dimension 0
- norm_gain: float32 [4096], replicated
- w_head: bfloat16 [4096, 128256], P(None, 'tp')
- draft_probs: float32 [128, 4, 128256], P('dp', None, 'tp'), parts along dimension 0
- draft_tokens: int32 [128, 4], P('dp'), parts along dimension 0
- temperature: float32 [128], P('dp'), parts along dimension 0
Outputs:
- output 1: float32 [128, 4], P('dp'), parts along dimension 0
- output 2: float32 [128, 4], P('dp'), parts along dimension 0
- output 3: float32 [128, 4, 128256], P('dp', None, 'tp'), parts along dimension 0
- output 4: float32 [128], P('dp'), parts along dimension 0
There are 2 independent parts. The reference program is written for one: setup_inputs(seed, part) draws one part's arguments, and reference() takes and returns one part's arrays. A program takes and returns all parts, laid end to end along the dimension named above; an argument that names none is the same for every part.
All inputs are finite; a program needn't handle non-finite values.
Results may differ from the reference program's by a relative error of at most 0.001.
Values sent between devices are 32-bit elements.
A program may use at most 1 GiB of HBM per device.

```python
import jax
import jax.numpy as jnp
from jax import lax

BATCH_ROWS = 64
DRAFT_LEN = 4
D_MODEL = 4096
VOCAB_SIZE = 128256
CLUSTER_COUNT = 3
WEIGHT_BLOCK = 128
CLUSTER_SPAN = VOCAB_SIZE // 32


def setup_inputs(seed: int = 0, part: int = 0) -> dict:
    part_key = jax.random.fold_in(jax.random.key(seed), part)
    key_h, key_q, key_s, key_t, key_c, key_k, key_o = jax.random.split(part_key, 7)
    key_w, key_g = jax.random.split(jax.random.key(seed + 1), 2)
    hidden = jax.random.normal(key_h, (BATCH_ROWS, DRAFT_LEN + 1, D_MODEL), jnp.float32).astype(jnp.bfloat16)
    norm_gain = jax.random.uniform(key_g, (D_MODEL,), jnp.float32, 0.5, 1.5)

    def weight_block(block_idx):
        gauss_block = jax.random.normal(jax.random.fold_in(key_w, block_idx), (WEIGHT_BLOCK, VOCAB_SIZE), jnp.float32)
        return (gauss_block * D_MODEL ** -0.5).astype(jnp.bfloat16)

    w_head = lax.map(weight_block, jnp.arange(D_MODEL // WEIGHT_BLOCK)).reshape(D_MODEL, VOCAB_SIZE)
    q_scale = jax.random.uniform(key_s, (BATCH_ROWS, DRAFT_LEN, 1), jnp.float32, 0.7, 1.3)
    q_logits = jax.random.normal(key_q, (BATCH_ROWS, DRAFT_LEN, VOCAB_SIZE), jnp.float32) * q_scale
    draft_probs = jax.nn.softmax(q_logits, axis=-1)
    temperature = jax.random.uniform(key_t, (BATCH_ROWS,), jnp.float32, 0.6, 1.4)
    centers = jax.random.randint(key_c, (CLUSTER_COUNT,), 0, VOCAB_SIZE - CLUSTER_SPAN)
    choice = jax.random.randint(key_k, (BATCH_ROWS, DRAFT_LEN), 0, CLUSTER_COUNT)
    offsets = jax.random.randint(key_o, (BATCH_ROWS, DRAFT_LEN), 0, CLUSTER_SPAN)
    draft_tokens = (centers[choice] + offsets).astype(jnp.int32)
    return {'hidden': hidden, 'norm_gain': norm_gain, 'w_head': w_head, 'draft_probs': draft_probs, 'draft_tokens': draft_tokens, 'temperature': temperature}


def reference(hidden, norm_gain, w_head, draft_probs, draft_tokens, temperature):
    def one_row(row_args):
        row_hidden, row_probs, row_tokens, row_temp = row_args
        hidden_f32 = row_hidden.astype(jnp.float32)
        inv_rms = lax.rsqrt(jnp.mean(hidden_f32 * hidden_f32, axis=-1, keepdims=True) + 1e-5)
        normed = (hidden_f32 * inv_rms * norm_gain).astype(jnp.bfloat16)
        logits = jnp.dot(normed, w_head, preferred_element_type=jnp.float32)
        scaled = logits / row_temp
        row_max = jnp.max(scaled, axis=-1, keepdims=True)
        row_lse = row_max + jnp.log(jnp.sum(jnp.exp(scaled - row_max), axis=-1, keepdims=True))
        target = jnp.exp(scaled[:DRAFT_LEN] - row_lse[:DRAFT_LEN])
        tok_target = jnp.take_along_axis(target, row_tokens[:, None], axis=-1)[:, 0]
        tok_draft = jnp.take_along_axis(row_probs, row_tokens[:, None], axis=-1)[:, 0]
        accept = jnp.minimum(1.0, tok_target / tok_draft)
        excess = jnp.maximum(target - row_probs, 0.0)
        norm_sum = jnp.sum(excess, axis=-1)
        residual = excess / norm_sum[:, None]
        return accept, norm_sum, residual, row_lse[DRAFT_LEN, 0]

    accept, norm_sum, residual, bonus_lse = lax.map(one_row, (hidden, draft_probs, draft_tokens, temperature))
    return accept, norm_sum, residual, bonus_lse
```

```python
import functools

import jax
import jax.numpy as jnp
from jax import lax
from jax.experimental import pallas as pl
from jax.experimental.pallas import tpu as pltpu
from jax.sharding import PartitionSpec as P

MESH = pl.DeviceIdType.MESH
F32 = jnp.float32
BF16 = jnp.bfloat16
LOG2E = 1.4426950408889634
LN2 = 0.6931471805599453
NEG = -1e30
LANES = 128
TILE = 256
BLOCK = 2 * TILE
SLOTS = 6
PIECE = 64


def stream_trips(vocab):
    return vocab // (2 * BLOCK)


def column(row):
    return jnp.transpose(jnp.broadcast_to(row, (LANES, LANES)))


def stream_kernel(dims, hid_ref, gain_ref, wt_ref, q_ref, meta_ref,
                  qb, zs, xb, wtail, mx, sm, tk, tokc, invc,
                  hid, xs, ring, hid_sem, w_sem, q_sem, t_sem):
    seqs, draft, depth, vocab = dims
    rows = seqs * draft
    total = rows + seqs
    ktiles = depth // TILE
    trips = stream_trips(vocab)
    nblocks = 2 * trips
    tail = vocab - nblocks * BLOCK
    pieces = total // PIECE

    def w_copy(block):
        slot = lax.rem(block, SLOTS)
        return pltpu.make_async_copy(
            wt_ref.at[pl.ds(pl.multiple_of(block * BLOCK, BLOCK), BLOCK), :], ring.at[slot], w_sem.at[slot])

    tail_copy = pltpu.make_async_copy(wt_ref.at[pl.ds(nblocks * BLOCK, tail), :], wtail, t_sem)

    hid_copy = pltpu.make_async_copy(hid_ref, hid, hid_sem)
    hid_copy.start()
    for i in range(SLOTS):
        w_copy(i).start()

    mx[...] = jnp.full(mx.shape, NEG, F32)
    sm[...] = jnp.ones(sm.shape, F32)
    tk[...] = jnp.zeros(tk.shape, F32)
    invc[pl.ds(0, LANES), :] = column(meta_ref[0:1, :])
    invc[pl.ds(LANES, LANES), :] = column(meta_ref[1:2, :])
    invc[pl.ds(2 * LANES, PIECE), :] = column(meta_ref[2:3, :])[0:PIECE, :]
    tokc[pl.ds(0, LANES), :] = column(meta_ref[3:4, :])
    tokc[pl.ds(LANES, LANES), :] = column(meta_ref[4:5, :])

    hid_copy.wait()
    chunks = depth // LANES

    def squares(c, accs):
        out = []
        for j in range(draft + 1):
            h = hid[j, :, pl.ds(pl.multiple_of(c * LANES, LANES), LANES)].astype(F32)
            out.append(accs[j] + h * h)
        return tuple(out)

    sums = lax.fori_loop(0, chunks, squares, tuple(jnp.zeros((seqs, LANES), F32) for _ in range(draft + 1)))
    invr = [jnp.broadcast_to(lax.rsqrt(jnp.sum(s, axis=-1, keepdims=True) * (1.0 / depth) + 1e-5), (seqs, LANES))
            for s in sums]

    def normalise(c, carry):
        lanes = pl.ds(pl.multiple_of(c * LANES, LANES), LANES)
        g = gain_ref[:, lanes]
        slab = lax.rem(c, 2)
        for j in range(draft + 1):
            x = hid[j, :, lanes].astype(F32) * carry[j] * g
            if j < draft:
                xs[slab, pl.ds(j, seqs, stride=draft), :] = x
            else:
                xs[slab, pl.ds(rows, seqs), :] = x
        xb[:, lanes] = xs[slab].astype(BF16)
        return carry

    lax.fori_loop(0, chunks, normalise, tuple(invr))

    lane = lax.broadcasted_iota(jnp.int32, (8, LANES), 1)

    per = 8

    def stream(*accs):
        acc = [[accs[(par * 2 + q) * pieces:(par * 2 + q + 1) * pieces] for q in range(2)] for par in range(2)]

        def push(slot, k, q):
            pltpu.matmul_push_rhs(ring[slot, q * TILE:(q + 1) * TILE, k * TILE:(k + 1) * TILE],
                                  staging_register=k % 2, mxu_index=q, transpose=True)

        def process(par, block):
            limit = jnp.where(block < 0, 0, BLOCK)
            base = block * BLOCK
            for p in range(pieces):
                z = [pltpu.matmul_pop(acc[par][q][p]) for q in range(2)]
                r = pl.ds(p * PIECE, PIECE)
                inv = invc[r, :]
                s = []
                for g in range(4):
                    v = z[g // 2][:, (g % 2) * LANES:(g % 2 + 1) * LANES] * inv
                    ok = jnp.broadcast_to((lane + g * LANES < limit)[0:1], (PIECE, LANES))
                    v = jnp.where(ok, v, NEG)
                    s.append(v)
                if (p + 1) * PIECE <= rows:
                    t = tk[r, :]
                    tokr = tokc[r, :]
                    for g in range(4):
                        col = (lane + (base + g * LANES)).astype(F32)[0:1]
                        t = t + jnp.where(tokr == col, s[g], 0.0)
                        zs[r, pl.ds(pl.multiple_of((block + 1) * BLOCK + g * LANES, LANES), LANES)] = s[g]
                    tk[r, :] = t
                m_old = mx[r, :]
                m_new = jnp.maximum(jnp.maximum(m_old, jnp.maximum(s[0], s[1])), jnp.maximum(s[2], s[3]))
                e = sm[r, :] * jnp.exp2(m_old - m_new)
                e = e + ((jnp.exp2(s[0] - m_new) + jnp.exp2(s[1] - m_new))
                         + (jnp.exp2(s[2] - m_new) + jnp.exp2(s[3] - m_new)))
                mx[r, :] = m_new
                sm[r, :] = e

        def half(trip, par):
            block = trip * 2 + par
            slot = lax.rem(block, SLOTS)
            after = lax.rem(block + 1, SLOTS)
            for k in range(ktiles):
                if k == ktiles - 2:
                    if par == 0:
                        w_copy(block + 1).wait()
                    else:
                        @pl.when(trip < trips - 1)
                        def _():
                            w_copy(block + 1).wait()
                    fresh = block - 1 + SLOTS

                    @pl.when((block >= 1) & (fresh < nblocks))
                    def _():
                        w_copy(fresh).start()

                    @pl.when(fresh == nblocks)
                    def _():
                        tail_copy.start()

                    @pl.when(block < seqs // per)
                    def _():
                        for i in range(per):
                            pltpu.make_async_copy(
                                q_ref.at[block * per + i],
                                qb.at[pl.ds(pl.multiple_of(block * per * draft, 8) + i * draft, draft), :],
                                q_sem.at[block * per + i]).start()
                for q in range(2):
                    if k + 1 < ktiles:
                        push(slot, k + 1, q)
                    else:
                        push(after, 0, q)
                for p in range(pieces):
                    x = xb[p * PIECE:(p + 1) * PIECE, k * TILE:(k + 1) * TILE]
                    for q in range(2):
                        pltpu.matmul_acc_lhs(acc[par][q][p], x, load_staged_rhs=(k % 2) if p == 0 else None)
                if k == 1:
                    process(1 - par, block - 1)

        for a in accs:
            pltpu.matmul_pop(a)
        w_copy(0).wait()
        for q in range(2):
            push(0, 0, q)

        @pl.loop(0, trips)
        def _(trip):
            half(trip, 0)
            half(trip, 1)

        zero = jnp.zeros((16, TILE), BF16)
        for q in range(2):
            pltpu.matmul_acc_lhs(acc[0][q][0], jnp.zeros((PIECE, TILE), BF16), load_staged_rhs=0)
        process(1, nblocks - 1)
        for q in range(2):
            pltpu.matmul_pop(acc[0][q][0])

    pl.run_scoped(stream, *[pltpu.ACC(q)((PIECE, TILE), F32)
                            for _ in range(2) for q in range(2) for _ in range(pieces)])

    tail_copy.wait()
    for b in range(seqs):
        pltpu.make_async_copy(q_ref.at[b], qb.at[pl.ds(b * draft, draft), :], q_sem.at[b]).wait()


def exchange_kernel(dims, n, q_ref, zs_ref, xb_ref, wtail_ref, mx_ref, sm_ref, tk_ref, tokc_ref, invc_ref, meta_ref,
                    zt, lcol, stat_ref, icol_ref,
                    mx, sm, tk, qcol, send1, recv1, send2, recv2, s1_sem, r1_sem, s2_sem, r2_sem):
    seqs, draft, depth, vocab = dims
    rows = seqs * draft
    total = rows + seqs
    me = lax.axis_index("tp")
    first_tail = 2 * stream_trips(vocab) * BLOCK
    tail = vocab - first_tail
    vtiles = pl.cdiv(vocab, LANES)
    lane = lax.broadcasted_iota(jnp.int32, (8, LANES), 1)

    barrier = pltpu.get_barrier_semaphore()
    for d in range(1, n):
        pl.semaphore_signal(barrier, inc=1, device_id={"tp": lax.rem(me + d, n)}, device_id_type=MESH)

    zt[:, :tail] = lax.dot_general(xb_ref[...], wtail_ref[...], (((1,), (1,)), ((), ())),
                                   preferred_element_type=F32)
    mx[...] = mx_ref[...]
    sm[...] = sm_ref[...]
    tk[...] = tk_ref[...]
    step = 32
    ttiles = pl.cdiv(tail, LANES)

    def finish(i, is_draft):
        r = pl.ds(pl.multiple_of(i * step, step), step)
        inv = invc_ref[r, :]
        s = []
        for g in range(ttiles):
            v = zt[r, g * LANES:(g + 1) * LANES] * inv
            if (g + 1) * LANES > tail:
                v = jnp.where(jnp.broadcast_to((lane + g * LANES < tail)[0:1], (step, LANES)), v, NEG)
            s.append(v)
        if is_draft:
            t = tk[r, :]
            tokr = tokc_ref[r, :]
            for g in range(ttiles):
                col = (lane + (first_tail + g * LANES)).astype(F32)[0:1]
                t = t + jnp.where(tokr == col, s[g], 0.0)
                zt[r, g * LANES:(g + 1) * LANES] = s[g]
            tk[r, :] = t
        m_old = mx[r, :]
        m_new = functools.reduce(jnp.maximum, s, m_old)
        e = sm[r, :] * jnp.exp2(m_old - m_new)
        for v in s:
            e = e + jnp.exp2(v - m_new)
        mx[r, :] = m_new
        sm[r, :] = e

    @pl.loop(0, rows // step)
    def _(i):
        finish(i, True)

    @pl.loop(rows // step, total // step)
    def _(i):
        finish(i, False)

    lse = []
    for blk in range(3):
        r = pl.ds(blk * LANES, LANES)
        mt = jnp.transpose(mx[r, :])
        st = jnp.transpose(sm[r, :])
        top = jnp.max(mt, axis=0, keepdims=True)
        tot = jnp.sum(st * jnp.exp2(mt - top), axis=0, keepdims=True)
        lse.append(top + jnp.log(tot) * LOG2E)
    for blk in range(3):
        send1[blk:blk + 1, :] = lse[blk]
        recv1[me, blk:blk + 1, :] = lse[blk]
    send1[3:4, :] = lse[2]
    recv1[me, 3:4, :] = lse[2]

    pl.semaphore_wait(barrier, n - 1)

    def exchange(send, recv, s_sem, r_sem):
        return [pltpu.make_async_remote_copy(
            src_ref=send, dst_ref=recv.at[me], send_sem=s_sem.at[d], recv_sem=r_sem.at[d],
            device_id={"tp": lax.rem(me + d, n)}, device_id_type=MESH) for d in range(1, n)]

    first = exchange(send1, recv1, s1_sem, r1_sem)
    for c in first:
        c.start()

    group = 32

    def gather(i, carry):
        r = pl.ds(pl.multiple_of(i * group, group), group)
        tokr = tokc_ref[r, :]
        acc = jnp.zeros((group, LANES), F32)
        for v in range(vtiles):
            size = min(LANES, vocab - v * LANES)
            col = (lane + v * LANES).astype(F32)[0:1]
            if size == LANES:
                acc = acc + jnp.where(tokr == col, q_ref[r, v * LANES:(v + 1) * LANES], 0.0)
            else:
                acc_t = jnp.where(tokr[:, :size] == col[:, :size], q_ref[r, v * LANES:v * LANES + size], 0.0)
                acc = acc + jnp.pad(acc_t, ((0, 0), (0, LANES - size)))
        qcol[r, :] = acc
        return carry

    lax.fori_loop(0, rows // group, gather, 0)
    tok_q = [jnp.sum(jnp.transpose(qcol[pl.ds(i * LANES, LANES), :]), axis=0, keepdims=True) for i in range(2)]
    tok_s = [jnp.sum(jnp.transpose(tk[pl.ds(i * LANES, LANES), :]), axis=0, keepdims=True) for i in range(2)]

    for c in first:
        c.wait()

    parts = [recv1[i] for i in range(n)]
    top = functools.reduce(jnp.maximum, parts)
    tot = functools.reduce(jnp.add, [jnp.exp2(x - top) for x in parts])
    full = top + jnp.log(tot) * LOG2E
    for i in range(2):
        lcol[pl.ds(i * LANES, LANES), :] = column(full[i:i + 1, :])

    def excess(i, carry):
        r = pl.ds(pl.multiple_of(i * group, group), group)
        lr = lcol[r, :]
        acc = jnp.zeros((group, LANES), F32)
        for v in range(vtiles):
            size = min(LANES, vocab - v * LANES)
            off = v * LANES - first_tail
            s = zs_ref[r, BLOCK + v * LANES:BLOCK + (v + 1) * LANES] if off < 0 else zt[r, off:off + LANES]
            e = jnp.maximum(jnp.exp2(s - lr)[:, :size] - q_ref[r, v * LANES:v * LANES + size], 0.0)
            acc = acc + (e if size == LANES else jnp.pad(e, ((0, 0), (0, LANES - size))))
        tk[r, :] = acc
        return carry

    lax.fori_loop(0, rows // group, excess, 0)

    for i in range(2):
        part = jnp.sum(jnp.transpose(tk[pl.ds(i * LANES, LANES), :]), axis=0, keepdims=True)
        tok = meta_ref[3 + i:4 + i, :]
        owned = (tok >= 0.0) & (tok < float(vocab))
        ratio = jnp.minimum(1.0, jnp.exp2(tok_s[i] - full[i:i + 1, :]) / jnp.where(owned, tok_q[i], 1.0))
        ratio = jnp.where(owned, ratio, 0.0)
        send2[i:i + 1, :] = part
        send2[2 + i:3 + i, :] = ratio
        recv2[me, i:i + 1, :] = part
        recv2[me, 2 + i:3 + i, :] = ratio

    second = exchange(send2, recv2, s2_sem, r2_sem)
    for c in second:
        c.start()
    for c in second:
        c.wait()
    summed = functools.reduce(jnp.add, [recv2[i] for i in range(n)])
    stat_ref[0:4, :] = summed
    stat_ref[4:8, :] = full * LN2
    for i in range(2):
        icol_ref[pl.ds(i * LANES, LANES), :] = column(1.0 / summed[i:i + 1, :])


def write_kernel(dims, q_ref, zs_ref, zt_ref, lcol_ref, icol_ref, out_ref, stage, sem):
    seqs, draft, depth, vocab = dims
    rows = seqs * draft
    vtiles = pl.cdiv(vocab, LANES)
    first_tail = 2 * stream_trips(vocab) * BLOCK
    group = 32
    per = group // draft

    def copy(b, row):
        return pltpu.make_async_copy(stage.at[pl.ds(row, draft), :], out_ref.at[b], sem.at[b])

    @pl.loop(0, rows // group)
    def _(i):
        base = pl.multiple_of(i * group, group)
        r = pl.ds(base, group)
        inv = icol_ref[r, :]
        lr = lcol_ref[r, :]
        for v in range(vtiles):
            size = min(LANES, vocab - v * LANES)
            off = v * LANES - first_tail
            s = zs_ref[r, BLOCK + v * LANES:BLOCK + (v + 1) * LANES] if off < 0 else zt_ref[r, off:off + LANES]
            e = jnp.maximum(jnp.exp2(s - lr)[:, :size] - q_ref[r, v * LANES:v * LANES + size], 0.0)
            stage[r, v * LANES:v * LANES + size] = e * inv[:, :size]
        for b in range(per):
            copy(i * per + b, base + b * draft).start()

    for b in range(seqs):
        copy(b, b * draft).wait()


def solution(mesh):
    n = mesh.shape["tp"]

    def local_step(hidden, norm_gain, w_head, draft_probs, draft_tokens, temperature):
        seqs, draft, vocab = draft_probs.shape
        depth = w_head.shape[0]
        dims = (seqs, draft, depth, vocab)
        rows = seqs * draft
        total = rows + seqs
        me = lax.axis_index("tp")

        inv_t = LOG2E / temperature
        tok = (draft_tokens - me * vocab).astype(F32).reshape(rows)
        meta = jnp.concatenate([jnp.repeat(inv_t, draft), inv_t, jnp.zeros((LANES - seqs,), F32), tok,
                                jnp.zeros((3 * LANES,), F32)]).reshape(8, LANES)
        vmem = pl.BlockSpec(memory_space=pltpu.VMEM)
        hbm = pl.BlockSpec(memory_space=pl.ANY)
        ttail = vocab - 2 * stream_trips(vocab) * BLOCK
        zwide = (2 * stream_trips(vocab) + 1) * BLOCK
        streamed = pl.pallas_call(
            functools.partial(stream_kernel, dims),
            out_shape=(pltpu.VMEM((rows, vocab), F32), pltpu.VMEM((rows, zwide), F32),
                       pltpu.VMEM((total, depth), BF16), pltpu.VMEM((ttail, depth), BF16),
                       pltpu.VMEM((3 * LANES, LANES), F32), pltpu.VMEM((3 * LANES, LANES), F32),
                       pltpu.VMEM((rows, LANES), F32), pltpu.VMEM((rows, LANES), F32),
                       pltpu.VMEM((total, LANES), F32)),
            in_specs=[hbm, vmem, hbm, hbm, vmem],
            out_specs=(vmem,) * 9,
            scratch_shapes=[
                pltpu.VMEM((draft + 1, seqs, depth), BF16),
                pltpu.VMEM((2, total, LANES), F32),
                pltpu.VMEM((SLOTS, BLOCK, depth), BF16),
                pltpu.SemaphoreType.DMA,
                pltpu.SemaphoreType.DMA((SLOTS,)),
                pltpu.SemaphoreType.DMA((seqs,)),
                pltpu.SemaphoreType.DMA,
            ],
            compiler_params=pltpu.CompilerParams(vmem_limit_bytes=30 * 1024 * 1024),
            name="verify_stream",
        )(jnp.transpose(hidden, (1, 0, 2)), norm_gain.reshape(1, depth), w_head.T, draft_probs, meta)

        streamed = [pltpu.with_memory_space_constraint(x, pltpu.VMEM) for x in streamed]
        twide = pl.cdiv(ttail, LANES) * LANES
        shared = pl.pallas_call(
            functools.partial(exchange_kernel, dims, n),
            out_shape=(pltpu.VMEM((total, twide), F32), pltpu.VMEM((rows, LANES), F32),
                       jax.ShapeDtypeStruct((8, LANES), F32), pltpu.VMEM((rows, LANES), F32)),
            in_specs=[vmem] * 10,
            out_specs=(vmem,) * 4,
            scratch_shapes=[
                pltpu.VMEM((3 * LANES, LANES), F32),
                pltpu.VMEM((3 * LANES, LANES), F32),
                pltpu.VMEM((rows, LANES), F32),
                pltpu.VMEM((rows, LANES), F32),
                pltpu.VMEM((4, LANES), F32),
                pltpu.VMEM((n, 4, LANES), F32),
                pltpu.VMEM((4, LANES), F32),
                pltpu.VMEM((n, 4, LANES), F32),
                pltpu.SemaphoreType.DMA((n,)),
                pltpu.SemaphoreType.DMA((n,)),
                pltpu.SemaphoreType.DMA((n,)),
                pltpu.SemaphoreType.DMA((n,)),
            ],
            compiler_params=pltpu.CompilerParams(
                collective_id=0, has_side_effects=True, vmem_limit_bytes=6 * 1024 * 1024),
            name="verify_exchange",
        )(*streamed, meta)
        zt, lcol, stat, icol = shared

        residual = pl.pallas_call(
            functools.partial(write_kernel, dims),
            out_shape=jax.ShapeDtypeStruct((seqs, draft, vocab), F32),
            in_specs=[vmem] * 5,
            out_specs=hbm,
            scratch_shapes=[pltpu.VMEM((rows, vocab), F32), pltpu.SemaphoreType.DMA((seqs,))],
            compiler_params=pltpu.CompilerParams(vmem_limit_bytes=10 * 1024 * 1024),
            name="verify_write",
        )(streamed[0], streamed[1], *[pltpu.with_memory_space_constraint(x, pltpu.VMEM) for x in (zt, lcol, icol)])

        norm_sum = stat[0:2].reshape(seqs, draft)
        accept = stat[2:4].reshape(seqs, draft)
        bonus = stat[6, :seqs]
        return accept, norm_sum, residual, bonus

    return jax.shard_map(
        local_step,
        mesh=mesh,
        in_specs=(P('dp', None, None), P(), P(None, 'tp'), P('dp', None, 'tp'), P('dp', None), P('dp')),
        out_specs=(P('dp', None), P('dp', None), P('dp', None, 'tp'), P('dp')),
        check_vma=False,
    )
```

```python
import functools

import jax
import jax.numpy as jnp
from jax import lax
from jax.experimental import pallas as pl
from jax.experimental.pallas import tpu as pltpu
from jax.sharding import PartitionSpec as P

MESH = pl.DeviceIdType.MESH
F32 = jnp.float32
BF16 = jnp.bfloat16
LOG2E = 1.4426950408889634
LN2 = 0.6931471805599453
NEG = -1e30
LANES = 128
TILE = 256
BLOCK = 2 * TILE
SLOTS = 6
PIECE = 64


def stream_blocks(vocab):
    return 2 * (vocab // (2 * BLOCK))


def column(row):
    return jnp.transpose(jnp.broadcast_to(row, (LANES, LANES)))


def stream_kernel(dims, hid_ref, gain_ref, wt_ref, temp_ref, tok_ref,
                  zs, xb, wtail, mx, sm, tokc, invc,
                  hid, xs, ring, row, hid_sem, w_sem, t_sem):
    seqs, draft, depth, vocab = dims
    rows = seqs * draft
    total = rows + seqs
    ktiles = depth // TILE
    nblocks = stream_blocks(vocab)
    tail = vocab - nblocks * BLOCK
    pieces = total // PIECE
    chunks = depth // LANES

    def w_copy(block):
        slot = lax.rem(block, SLOTS)
        return pltpu.make_async_copy(
            wt_ref.at[pl.ds(pl.multiple_of(block * BLOCK, BLOCK), BLOCK), :], ring.at[slot], w_sem.at[slot])

    tail_copy = pltpu.make_async_copy(wt_ref.at[pl.ds(nblocks * BLOCK, tail), :], wtail, t_sem)
    hid_copies = [pltpu.make_async_copy(hid_ref.at[j], hid.at[j], hid_sem.at[j]) for j in range(draft + 1)]
    for c in hid_copies:
        c.start()
    for i in range(SLOTS):
        w_copy(i).start(priority=1)

    mx[...] = jnp.full(mx.shape, NEG, F32)
    sm[...] = jnp.ones(sm.shape, F32)
    row[...] = jnp.ones(row.shape, F32)
    row[0:1, 0:seqs] = temp_ref[...]
    row[1:1 + draft, 0:seqs] = (tok_ref[...] - lax.axis_index("tp") * vocab).astype(F32)
    inv = LOG2E / column(row[0:1, :])[0:seqs, :]
    for j in range(draft):
        invc[pl.ds(j, seqs, stride=draft), :] = inv
        tokc[pl.ds(j, seqs, stride=draft), :] = column(row[1 + j:2 + j, :])[0:seqs, :]
    invc[pl.ds(rows, seqs), :] = inv

    invr = []
    for j in range(draft + 1):
        hid_copies[j].wait()

        def squares(c, acc, j=j):
            out = []
            for u in range(4):
                h = hid[j, :, pl.ds(pl.multiple_of((c * 4 + u) * LANES, LANES), LANES)].astype(F32)
                out.append(h * h)
            return acc + ((out[0] + out[1]) + (out[2] + out[3]))

        s = lax.fori_loop(0, chunks // 4, squares, jnp.zeros((seqs, LANES), F32))
        r = lax.rsqrt(jnp.sum(s, axis=-1, keepdims=True) * (1.0 / depth) + 1e-5)
        invr.append(jnp.broadcast_to(r, (seqs, LANES)))

    def normalise(c, carry):
        for u in range(2):
            lanes = pl.ds(pl.multiple_of((c * 2 + u) * LANES, LANES), LANES)
            g = gain_ref[:, lanes]
            for j in range(draft + 1):
                x = hid[j, :, lanes].astype(F32) * carry[j] * g
                if j < draft:
                    xs[u, pl.ds(j, seqs, stride=draft), :] = x
                else:
                    xb[pl.ds(rows, seqs), lanes] = x.astype(BF16)
        for u in range(2):
            lanes = pl.ds(pl.multiple_of((c * 2 + u) * LANES, LANES), LANES)
            xb[pl.ds(0, rows), lanes] = xs[u].astype(BF16)
        return carry

    lax.fori_loop(0, chunks // 2, normalise, tuple(invr))

    def stream(*accs):
        acc = [[accs[(par * 2 + q) * pieces:(par * 2 + q + 1) * pieces] for q in range(2)] for par in range(2)]

        def push(slot, k, q):
            pltpu.matmul_push_rhs(ring[slot, q * TILE:(q + 1) * TILE, k * TILE:(k + 1) * TILE],
                                  staging_register=k % 2, mxu_index=q, transpose=True)

        def process(par, block):
            for p in range(pieces):
                z = [pltpu.matmul_pop(acc[par][q][p]) for q in range(2)]
                r = pl.ds(p * PIECE, PIECE)
                inv = invc[r, :]
                s = [z[g // 2][:, (g % 2) * LANES:(g % 2 + 1) * LANES] * inv for g in range(4)]
                if (p + 1) * PIECE <= rows:
                    for g in range(4):
                        zs[r, pl.ds(pl.multiple_of(block * BLOCK + g * LANES, LANES), LANES)] = s[g]
                m_old = mx[r, :]
                m_new = jnp.maximum(jnp.maximum(m_old, jnp.maximum(s[0], s[1])), jnp.maximum(s[2], s[3]))
                e = sm[r, :] * jnp.exp2(m_old - m_new)
                e = e + ((jnp.exp2(s[0] - m_new) + jnp.exp2(s[1] - m_new))
                         + (jnp.exp2(s[2] - m_new) + jnp.exp2(s[3] - m_new)))
                mx[r, :] = m_new
                sm[r, :] = e

        def half(block, par, first=False, last=False, fetch=False):
            slot = lax.rem(block, SLOTS)
            after = lax.rem(block + 1, SLOTS)
            if not last:
                w_copy(block + 1).wait()
            if fetch:
                w_copy(block - 1 + SLOTS).start(priority=1)
            for k in range(ktiles):
                for q in range(2):
                    if k + 1 < ktiles:
                        push(slot, k + 1, q)
                    elif not last:
                        push(after, 0, q)
                for p in range(pieces):
                    x = xb[p * PIECE:(p + 1) * PIECE, k * TILE:(k + 1) * TILE]
                    for q in range(2):
                        pltpu.matmul_acc_lhs(acc[par][q][p], x, load_staged_rhs=(k % 2) if p == 0 else None)
                if k == 1 and not first:
                    process(1 - par, block - 1)

        for a in accs:
            pltpu.matmul_pop(a)
        w_copy(0).wait()
        for q in range(2):
            push(0, 0, q)
        half(0, 0, first=True)
        steady = (nblocks - SLOTS) // 2

        @pl.loop(0, steady)
        def _(trip):
            half(trip * 2 + 1, 1, fetch=True)
            half(trip * 2 + 2, 0, fetch=True)

        tail_copy.start(priority=1)

        @pl.loop(steady, (nblocks - 2) // 2)
        def _(trip):
            half(trip * 2 + 1, 1)
            half(trip * 2 + 2, 0)

        half(nblocks - 1, 1, last=True)
        process(1, nblocks - 1)

    pl.run_scoped(stream, *[pltpu.ACC(q)((PIECE, TILE), F32)
                            for _ in range(2) for q in range(2) for _ in range(pieces)])
    tail_copy.wait()


def exchange_kernel(dims, n, q_hbm, zs_ref, xb_ref, wtail_ref, mx_ref, sm_ref, tokc_ref, invc_ref, tok_ref,
                    q_ref, zt, lcol, icol, stat,
                    mx, sm, ta, tb, own, send1, recv1, send2, recv2, q_sem, s1_sem, r1_sem, s2_sem, r2_sem):
    seqs, draft, depth, vocab = dims
    rows = seqs * draft
    total = rows + seqs
    me = lax.axis_index("tp")
    first_tail = stream_blocks(vocab) * BLOCK
    tail = vocab - first_tail
    vtiles = pl.cdiv(vocab, LANES)
    ttiles = pl.cdiv(tail, LANES)
    lane = lax.broadcasted_iota(jnp.int32, (8, LANES), 1)
    half = seqs

    barrier = pltpu.get_barrier_semaphore()
    for d in range(1, n):
        pl.semaphore_signal(barrier, inc=1, device_id={"tp": lax.rem(me + d, n)}, device_id_type=MESH)

    q_copies = [pltpu.make_async_copy(q_hbm.at[b], q_ref.at[pl.ds(b * draft, draft), :], q_sem.at[b])
                for b in range(seqs)]
    for c in q_copies:
        c.start(priority=1)

    zt[:, :tail] = lax.dot_general(xb_ref[...], wtail_ref[...], (((1,), (1,)), ((), ())),
                                   preferred_element_type=F32)
    step = 32

    def finish(i, is_draft):
        r = pl.ds(pl.multiple_of(i * step, step), step)
        inv = invc_ref[r, :]
        s = []
        for g in range(ttiles):
            v = zt[r, g * LANES:(g + 1) * LANES] * inv
            if (g + 1) * LANES > tail:
                v = jnp.where(jnp.broadcast_to((lane + g * LANES < tail)[0:1], (step, LANES)), v, NEG)
            s.append(v)
        if is_draft:
            for g in range(ttiles):
                zt[r, g * LANES:(g + 1) * LANES] = s[g]
        m_old = mx_ref[r, :]
        m_new = functools.reduce(jnp.maximum, s, m_old)
        e = sm_ref[r, :] * jnp.exp2(m_old - m_new)
        for v in s:
            e = e + jnp.exp2(v - m_new)
        mx[r, :] = m_new
        sm[r, :] = e

    @pl.loop(0, rows // step)
    def _(i):
        finish(i, True)

    @pl.loop(rows // step, total // step)
    def _(i):
        finish(i, False)

    def rows_of(ref, j):
        return ref[pl.ds(j, seqs, stride=draft), :]

    for j in range(draft):
        mt = jnp.transpose(jnp.concatenate([rows_of(mx, j), mx[pl.ds(rows, seqs), :]], axis=0))
        st = jnp.transpose(jnp.concatenate([rows_of(sm, j), sm[pl.ds(rows, seqs), :]], axis=0))
        top = jnp.max(mt, axis=0, keepdims=True)
        tot = jnp.sum(st * jnp.exp2(mt - top), axis=0, keepdims=True)
        lse = top + jnp.log(tot) * LOG2E
        send1[j:j + 1, :] = lse
        recv1[me, j:j + 1, :] = lse

    pl.semaphore_wait(barrier, n - 1)

    def exchange(send, recv, s_sem, r_sem):
        return [pltpu.make_async_remote_copy(
            src_ref=send, dst_ref=recv.at[me], send_sem=s_sem.at[d], recv_sem=r_sem.at[d],
            device_id={"tp": lax.rem(me + d, n)}, device_id_type=MESH) for d in range(1, n)]

    first = exchange(send1, recv1, s1_sem, r1_sem)
    for c in first:
        c.start()

    own[...] = jnp.zeros(own.shape, jnp.int32)
    own[:, 0:seqs] = tok_ref[...] - me * vocab
    for c in q_copies:
        c.wait()

    group = 32

    def scaled(r, v):
        off = v * LANES - first_tail
        return zs_ref[r, v * LANES:(v + 1) * LANES] if off < 0 else zt[r, off:off + LANES]

    def gather(i, carry):
        r = pl.ds(pl.multiple_of(i * group, group), group)
        tokr = tokc_ref[r, :]
        acc_s = jnp.zeros((group, LANES), F32)
        acc_q = jnp.zeros((group, LANES), F32)
        for v in range(vtiles):
            size = min(LANES, vocab - v * LANES)
            hit = tokr == (lane + v * LANES).astype(F32)[0:1]
            acc_s = acc_s + jnp.where(hit, scaled(r, v), 0.0)
            if size == LANES:
                acc_q = acc_q + jnp.where(hit, q_ref[r, v * LANES:(v + 1) * LANES], 0.0)
            else:
                part = jnp.where(hit[:, :size], q_ref[r, v * LANES:v * LANES + size], 0.0)
                acc_q = acc_q + jnp.pad(part, ((0, 0), (0, LANES - size)))
        ta[r, :] = acc_s
        tb[r, :] = acc_q
        return carry

    lax.fori_loop(0, rows // group, gather, 0)
    picked = [jnp.sum(jnp.transpose(jnp.concatenate([rows_of(ta, j), rows_of(tb, j)], axis=0)),
                      axis=0, keepdims=True) for j in range(draft)]

    for c in first:
        c.wait()

    parts = [recv1[i] for i in range(n)]
    top = functools.reduce(jnp.maximum, parts)
    tot = functools.reduce(jnp.add, [jnp.exp2(x - top) for x in parts])
    full = top + jnp.log(tot) * LOG2E
    for j in range(draft):
        lcol[pl.ds(j, seqs, stride=draft), :] = column(full[j:j + 1, :])[0:seqs, :]

    def excess(i, carry):
        r = pl.ds(pl.multiple_of(i * group, group), group)
        lr = lcol[r, :]
        acc = jnp.zeros((group, LANES), F32)
        for v in range(vtiles):
            size = min(LANES, vocab - v * LANES)
            e = jnp.maximum(jnp.exp2(scaled(r, v) - lr)[:, :size] - q_ref[r, v * LANES:v * LANES + size], 0.0)
            acc = acc + (e if size == LANES else jnp.pad(e, ((0, 0), (0, LANES - size))))
        ta[r, :] = acc
        return carry

    lax.fori_loop(0, rows // group, excess, 0)

    for j in range(draft):
        part = jnp.sum(jnp.transpose(jnp.concatenate([rows_of(ta, j), rows_of(ta, j)], axis=0)),
                       axis=0, keepdims=True)
        tok = own[j:j + 1, :]
        owned = (tok >= 0) & (tok < vocab)
        ratio = jnp.minimum(1.0, jnp.exp2(picked[j] - full[j:j + 1, :])
                            / jnp.where(owned, pltpu.roll(picked[j], half, 1), 1.0))
        ratio = jnp.where(owned, ratio, 0.0)
        both = jnp.where(lane[0:1] < half, part, pltpu.roll(ratio, half, 1))
        send2[j:j + 1, :] = both
        recv2[me, j:j + 1, :] = both

    second = exchange(send2, recv2, s2_sem, r2_sem)
    for c in second:
        c.start()
    for c in second:
        c.wait()
    summed = functools.reduce(jnp.add, [recv2[i] for i in range(n)])
    stat[0:4, :] = summed
    stat[4:8, :] = pltpu.roll(full * LN2, half, 1)
    for j in range(draft):
        icol[pl.ds(j, seqs, stride=draft), :] = column(1.0 / summed[j:j + 1, :])[0:seqs, :]


def write_kernel(dims, q_ref, zs_ref, zt_ref, lcol_ref, icol_ref, stat_ref,
                 out_ref, accept_ref, norm_ref, bonus_ref, stage, sem):
    seqs, draft, depth, vocab = dims
    rows = seqs * draft
    vtiles = pl.cdiv(vocab, LANES)
    first_tail = stream_blocks(vocab) * BLOCK
    group = 32
    per = group // draft

    def copy(b, row):
        return pltpu.make_async_copy(stage.at[pl.ds(row, draft), :], out_ref.at[b], sem.at[b])

    @pl.loop(0, rows // group)
    def _(i):
        base = pl.multiple_of(i * group, group)
        r = pl.ds(base, group)
        inv = icol_ref[r, :]
        lr = lcol_ref[r, :]
        for v in range(vtiles):
            size = min(LANES, vocab - v * LANES)
            off = v * LANES - first_tail
            s = zs_ref[r, v * LANES:(v + 1) * LANES] if off < 0 else zt_ref[r, off:off + LANES]
            e = jnp.maximum(jnp.exp2(s - lr)[:, :size] - q_ref[r, v * LANES:v * LANES + size], 0.0)
            stage[r, v * LANES:v * LANES + size] = e * inv[:, :size]
        for b in range(per):
            copy(i * per + b, base + b * draft).start(priority=1)

    norm_ref[...] = stat_ref[0:draft, 0:seqs]
    accept_ref[...] = pltpu.roll(stat_ref[0:draft, :], seqs, 1)[:, 0:seqs]
    bonus_ref[...] = stat_ref[4:5, 0:seqs]
    for b in range(seqs):
        copy(b, b * draft).wait()


def solution(mesh):
    n = mesh.shape["tp"]

    def local_step(hidden, norm_gain, w_head, draft_probs, draft_tokens, temperature):
        seqs, draft, vocab = draft_probs.shape
        depth = w_head.shape[0]
        dims = (seqs, draft, depth, vocab)
        rows = seqs * draft
        total = rows + seqs
        zwide = stream_blocks(vocab) * BLOCK
        ttail = vocab - zwide
        twide = pl.cdiv(ttail, LANES) * LANES
        vmem = pl.BlockSpec(memory_space=pltpu.VMEM)
        hbm = pl.BlockSpec(memory_space=pl.ANY)

        def held(xs):
            return [pltpu.with_memory_space_constraint(x, pltpu.VMEM) for x in xs]

        tokens = draft_tokens.T
        streamed = pl.pallas_call(
            functools.partial(stream_kernel, dims),
            out_shape=(pltpu.VMEM((rows, zwide), F32),
                       pltpu.VMEM((total, depth), BF16), pltpu.VMEM((ttail, depth), BF16),
                       pltpu.VMEM((total, LANES), F32), pltpu.VMEM((total, LANES), F32),
                       pltpu.VMEM((rows, LANES), F32), pltpu.VMEM((total, LANES), F32)),
            in_specs=[hbm, vmem, hbm, vmem, vmem],
            out_specs=(vmem,) * 7,
            scratch_shapes=[
                pltpu.VMEM((draft + 1, seqs, depth), BF16),
                pltpu.VMEM((2, rows, LANES), F32),
                pltpu.VMEM((SLOTS, BLOCK, depth), BF16),
                pltpu.VMEM((8, LANES), F32),
                pltpu.SemaphoreType.DMA((draft + 1,)),
                pltpu.SemaphoreType.DMA((SLOTS,)),
                pltpu.SemaphoreType.DMA,
            ],
            compiler_params=pltpu.CompilerParams(vmem_limit_bytes=30 * 1024 * 1024),
            name="verify_stream",
        )(pltpu.with_memory_space_constraint(jnp.transpose(hidden, (1, 0, 2)), pltpu.HBM), norm_gain.reshape(1, depth), w_head.T,
          temperature.reshape(1, seqs), tokens)
        zs = streamed[0]

        shared = pl.pallas_call(
            functools.partial(exchange_kernel, dims, n),
            out_shape=(pltpu.VMEM((rows, vocab), F32), pltpu.VMEM((total, twide), F32),
                       pltpu.VMEM((rows, LANES), F32), pltpu.VMEM((rows, LANES), F32),
                       pltpu.VMEM((8, LANES), F32)),
            in_specs=[hbm] + [vmem] * 8,
            out_specs=(vmem,) * 5,
            scratch_shapes=[
                pltpu.VMEM((total, LANES), F32),
                pltpu.VMEM((total, LANES), F32),
                pltpu.VMEM((rows, LANES), F32),
                pltpu.VMEM((rows, LANES), F32),
                pltpu.VMEM((draft, LANES), jnp.int32),
                pltpu.VMEM((4, LANES), F32),
                pltpu.VMEM((n, 4, LANES), F32),
                pltpu.VMEM((4, LANES), F32),
                pltpu.VMEM((n, 4, LANES), F32),
                pltpu.SemaphoreType.DMA((seqs,)),
                pltpu.SemaphoreType.DMA((n,)),
                pltpu.SemaphoreType.DMA((n,)),
                pltpu.SemaphoreType.DMA((n,)),
                pltpu.SemaphoreType.DMA((n,)),
            ],
            compiler_params=pltpu.CompilerParams(
                collective_id=0, has_side_effects=True, vmem_limit_bytes=6 * 1024 * 1024),
            name="verify_exchange",
        )(pltpu.with_memory_space_constraint(draft_probs, pltpu.HBM), *held(streamed), tokens)

        residual, accept, norm_sum, bonus = pl.pallas_call(
            functools.partial(write_kernel, dims),
            out_shape=(jax.ShapeDtypeStruct((seqs, draft, vocab), F32),
                       jax.ShapeDtypeStruct((draft, seqs), F32), jax.ShapeDtypeStruct((draft, seqs), F32),
                       jax.ShapeDtypeStruct((1, seqs), F32)),
            in_specs=[vmem] * 6,
            out_specs=(hbm, vmem, vmem, vmem),
            scratch_shapes=[pltpu.VMEM((rows, vocab), F32), pltpu.SemaphoreType.DMA((seqs,))],
            compiler_params=pltpu.CompilerParams(vmem_limit_bytes=10 * 1024 * 1024),
            name="verify_write",
        )(*held((shared[0], zs) + tuple(shared[1:])))

        return accept.T, norm_sum.T, residual, bonus.reshape(seqs)

    return jax.shard_map(
        local_step,
        mesh=mesh,
        in_specs=(P('dp', None, None), P(), P(None, 'tp'), P('dp', None, 'tp'), P('dp', None), P('dp')),
        out_specs=(P('dp', None), P('dp', None), P('dp', None, 'tp'), P('dp')),
        check_vma=False,
    )
```

```python
import functools

import jax
import jax.numpy as jnp
from jax import lax
from jax.experimental import pallas as pl
from jax.experimental.pallas import tpu as pltpu
from jax.sharding import PartitionSpec as P

MESH = pl.DeviceIdType.MESH
F32 = jnp.float32
BF16 = jnp.bfloat16
LOG2E = 1.4426950408889634
LN2 = 0.6931471805599453
NEG = -1e30
LANES = 128
TILE = 256
BLOCK = 2 * TILE
SLOTS = 6
PIECE = 64


def stream_blocks(vocab):
    return 2 * (vocab // (2 * BLOCK))


def column(row):
    return jnp.transpose(jnp.broadcast_to(row, (LANES, LANES)))


def stream_kernel(dims, hid_hbm, gain_hbm, wt_ref, temp_hbm, tok_hbm,
                  zs, xb, wtail, mx, sm, tokc, invc, own,
                  hid, xs, ring, row, gain_ref, temp_ref, tok_ref, rr, hid_sem, w_sem, t_sem, c_sem, f_sem):
    seqs, draft, depth, vocab = dims
    rows = seqs * draft
    total = rows + seqs
    ktiles = depth // TILE
    nblocks = stream_blocks(vocab)
    tail = vocab - nblocks * BLOCK
    pieces = total // PIECE
    chunks = depth // LANES

    def w_copy(block):
        slot = lax.rem(block, SLOTS)
        return pltpu.make_async_copy(
            wt_ref.at[pl.ds(pl.multiple_of(block * BLOCK, BLOCK), BLOCK), :], ring.at[slot], w_sem.at[slot])

    tail_copy = pltpu.make_async_copy(wt_ref.at[pl.ds(nblocks * BLOCK, tail), :], wtail, t_sem)
    hid_copies = [pltpu.make_async_copy(hid_hbm.at[j], hid.at[j], hid_sem.at[j]) for j in range(draft + 1)]
    small = [pltpu.make_async_copy(a, b, c_sem.at[i]) for i, (a, b) in enumerate(
        [(temp_hbm, temp_ref), (tok_hbm, tok_ref), (gain_hbm, gain_ref)])]
    for c in small + hid_copies:
        c.start()
    fold = depth // 2
    first_copies = [pltpu.make_async_copy(
        wt_ref.at[pl.ds(0, BLOCK), pl.ds(i * fold, fold)], ring.at[0, :, pl.ds(i * fold, fold)], f_sem.at[i])
        for i in range(2)]
    for c in first_copies:
        c.start(priority=1)
    for i in range(1, SLOTS):
        w_copy(i).start(priority=1)

    mx[...] = jnp.full(mx.shape, NEG, F32)
    sm[...] = jnp.ones(sm.shape, F32)
    row[...] = jnp.ones(row.shape, F32)
    own[...] = jnp.zeros(own.shape, jnp.int32)
    for c in small:
        c.wait()
    row[0:1, 0:seqs] = temp_ref[...]
    own[:, 0:seqs] = tok_ref[...] - lax.axis_index("tp") * vocab
    row[1:1 + draft, 0:seqs] = own[:, 0:seqs].astype(F32)
    inv = LOG2E / column(row[0:1, :])[0:seqs, :]
    for j in range(draft):
        invc[pl.ds(j, seqs, stride=draft), :] = inv
        tokc[pl.ds(j, seqs, stride=draft), :] = column(row[1 + j:2 + j, :])[0:seqs, :]
    invc[pl.ds(rows, seqs), :] = inv

    for j in range(draft + 1):
        hid_copies[j].wait()

        def squares(c, acc, j=j):
            for u in range(16):
                h = hid[j, :, pl.ds(pl.multiple_of((c * 16 + u) * LANES, LANES), LANES)].astype(F32)
                acc = acc + h * h
            return acc

        s = lax.fori_loop(0, chunks // 16, squares, jnp.zeros((seqs, LANES), F32))
        r = lax.rsqrt(jnp.sum(s, axis=-1, keepdims=True) * (1.0 / depth) + 1e-5)
        rr[j] = jnp.broadcast_to(r, (seqs, LANES))

    def normalise(k):
        for u in range(2):
            lanes = slice((k * 2 + u) * LANES, (k * 2 + u + 1) * LANES)
            slab = (k * 2 + u) % 4
            g = gain_ref[:, lanes]
            for j in range(draft + 1):
                x = hid[j, :, lanes].astype(F32) * rr[j] * g
                if j < draft:
                    xs[slab, pl.ds(j, seqs, stride=draft), :] = x
                else:
                    xb[pl.ds(rows, seqs), lanes] = x.astype(BF16)
            xb[pl.ds(0, rows), lanes] = xs[slab].astype(BF16)

    normalise(0)

    def stream(*accs):
        acc = [[accs[(par * 2 + q) * pieces:(par * 2 + q + 1) * pieces] for q in range(2)] for par in range(2)]

        def push(slot, k, q):
            pltpu.matmul_push_rhs(ring[slot, q * TILE:(q + 1) * TILE, k * TILE:(k + 1) * TILE],
                                  staging_register=k % 2, mxu_index=q, transpose=True)

        def process(par, block, which):
            for p in which:
                z = [pltpu.matmul_pop(acc[par][q][p]) for q in range(2)]
                r = pl.ds(p * PIECE, PIECE)
                inv = invc[r, :]
                s = [z[g // 2][:, (g % 2) * LANES:(g % 2 + 1) * LANES] * inv for g in range(4)]
                if (p + 1) * PIECE <= rows:
                    for g in range(4):
                        zs[r, pl.ds(pl.multiple_of(block * BLOCK + g * LANES, LANES), LANES)] = s[g]
                m_old = mx[r, :]
                m_new = jnp.maximum(jnp.maximum(m_old, jnp.maximum(s[0], s[1])), jnp.maximum(s[2], s[3]))
                e = sm[r, :] * jnp.exp2(m_old - m_new)
                e = e + ((jnp.exp2(s[0] - m_new) + jnp.exp2(s[1] - m_new))
                         + (jnp.exp2(s[2] - m_new) + jnp.exp2(s[3] - m_new)))
                mx[r, :] = m_new
                sm[r, :] = e

        def half(block, par, first=False, last=False, fetch=False):
            slot = lax.rem(block, SLOTS)
            after = lax.rem(block + 1, SLOTS)
            for k in range(ktiles):
                if first and k == ktiles // 2 - 1:
                    first_copies[1].wait()
                if k == ktiles - 1:
                    if not last:
                        w_copy(block + 1).wait()
                    if fetch:
                        w_copy(block - 1 + SLOTS).start(priority=1)
                if first and k + 1 < ktiles:
                    normalise(k + 1)
                for q in range(2):
                    if k + 1 < ktiles:
                        push(slot, k + 1, q)
                    elif not last:
                        push(after, 0, q)
                for p in range(pieces):
                    x = xb[p * PIECE:(p + 1) * PIECE, k * TILE:(k + 1) * TILE]
                    for q in range(2):
                        pltpu.matmul_acc_lhs(acc[par][q][p], x, load_staged_rhs=(k % 2) if p == 0 else None)
                if k % 2 == 1 and k // 2 < pieces and not first:
                    process(1 - par, block - 1, [k // 2])

        for c in first_copies[:1]:
            c.wait()
        for q in range(2):
            push(0, 0, q)
        half(0, 0, first=True)
        steady = (nblocks - SLOTS) // 2

        @pl.loop(0, steady)
        def _(trip):
            half(trip * 2 + 1, 1, fetch=True)
            half(trip * 2 + 2, 0, fetch=True)

        tail_copy.start(priority=1)

        @pl.loop(steady, (nblocks - 2) // 2)
        def _(trip):
            half(trip * 2 + 1, 1)
            half(trip * 2 + 2, 0)

        half(nblocks - 1, 1, last=True)
        process(1, nblocks - 1, range(pieces))

    pl.run_scoped(stream, *[pltpu.ACC(q)((PIECE, TILE), F32)
                            for _ in range(2) for q in range(2) for _ in range(pieces)])
    tail_copy.wait()


def exchange_kernel(dims, n, q_hbm, zs_ref, xb_ref, wtail_ref, mx_ref, sm_ref, tokc_ref, invc_ref, own,
                    q_ref, icol, stat,
                    zt, lcol, mx, sm, ta, tb, send1, recv1, send2, recv2, q_sem, s1_sem, r1_sem, s2_sem, r2_sem):
    seqs, draft, depth, vocab = dims
    rows = seqs * draft
    total = rows + seqs
    me = lax.axis_index("tp")
    first_tail = stream_blocks(vocab) * BLOCK
    tail = vocab - first_tail
    vtiles = pl.cdiv(vocab, LANES)
    ttiles = pl.cdiv(tail, LANES)
    lane = lax.broadcasted_iota(jnp.int32, (8, LANES), 1)
    half = seqs

    barrier = pltpu.get_barrier_semaphore()
    for d in range(1, n):
        pl.semaphore_signal(barrier, inc=1, device_id={"tp": lax.rem(me + d, n)}, device_id_type=MESH)

    q_copies = [pltpu.make_async_copy(q_hbm.at[b], q_ref.at[pl.ds(b * draft, draft), :], q_sem.at[b])
                for b in range(seqs)]
    for c in q_copies:
        c.start(priority=1)

    zt[:, :tail] = lax.dot_general(xb_ref[...], wtail_ref[...], (((1,), (1,)), ((), ())),
                                   preferred_element_type=F32)
    step = 32

    def finish(i, is_draft):
        r = pl.ds(pl.multiple_of(i * step, step), step)
        inv = invc_ref[r, :]
        s = []
        for g in range(ttiles):
            v = zt[r, g * LANES:(g + 1) * LANES] * inv
            if (g + 1) * LANES > tail:
                v = jnp.where(jnp.broadcast_to((lane + g * LANES < tail)[0:1], (step, LANES)), v, NEG)
            s.append(v)
        if is_draft:
            for g in range(ttiles):
                zt[r, g * LANES:(g + 1) * LANES] = s[g]
        m_old = mx_ref[r, :]
        m_new = functools.reduce(jnp.maximum, s, m_old)
        e = sm_ref[r, :] * jnp.exp2(m_old - m_new)
        for v in s:
            e = e + jnp.exp2(v - m_new)
        mx[r, :] = m_new
        sm[r, :] = e

    @pl.loop(0, rows // step)
    def _(i):
        finish(i, True)

    @pl.loop(rows // step, total // step)
    def _(i):
        finish(i, False)

    def rows_of(ref, j):
        return ref[pl.ds(j, seqs, stride=draft), :]

    for j in range(draft):
        mt = jnp.transpose(jnp.concatenate([rows_of(mx, j), mx[pl.ds(rows, seqs), :]], axis=0))
        st = jnp.transpose(jnp.concatenate([rows_of(sm, j), sm[pl.ds(rows, seqs), :]], axis=0))
        top = jnp.max(mt, axis=0, keepdims=True)
        tot = jnp.sum(st * jnp.exp2(mt - top), axis=0, keepdims=True)
        lse = top + jnp.log(tot) * LOG2E
        send1[j:j + 1, :] = lse
        recv1[me, j:j + 1, :] = lse

    pl.semaphore_wait(barrier, n - 1)

    def exchange(send, recv, s_sem, r_sem):
        return [pltpu.make_async_remote_copy(
            src_ref=send, dst_ref=recv.at[me], send_sem=s_sem.at[d], recv_sem=r_sem.at[d],
            device_id={"tp": lax.rem(me + d, n)}, device_id_type=MESH) for d in range(1, n)]

    first = exchange(send1, recv1, s1_sem, r1_sem)
    for c in first:
        c.start()

    for c in q_copies:
        c.wait()

    group = 32

    def scaled(r, v):
        off = v * LANES - first_tail
        return zs_ref[r, v * LANES:(v + 1) * LANES] if off < 0 else zt[r, off:off + LANES]

    def gather(i, carry):
        r = pl.ds(pl.multiple_of(i * group, group), group)
        tokr = tokc_ref[r, :]
        acc_s = jnp.zeros((group, LANES), F32)
        acc_q = jnp.zeros((group, LANES), F32)
        for v in range(vtiles):
            size = min(LANES, vocab - v * LANES)
            hit = tokr == (lane + v * LANES).astype(F32)[0:1]
            acc_s = acc_s + jnp.where(hit, scaled(r, v), 0.0)
            if size == LANES:
                acc_q = acc_q + jnp.where(hit, q_ref[r, v * LANES:(v + 1) * LANES], 0.0)
            else:
                part = jnp.where(hit[:, :size], q_ref[r, v * LANES:v * LANES + size], 0.0)
                acc_q = acc_q + jnp.pad(part, ((0, 0), (0, LANES - size)))
        ta[r, :] = acc_s
        tb[r, :] = acc_q
        return carry

    lax.fori_loop(0, rows // group, gather, 0)
    picked = [jnp.sum(jnp.transpose(jnp.concatenate([rows_of(ta, j), rows_of(tb, j)], axis=0)),
                      axis=0, keepdims=True) for j in range(draft)]

    for c in first:
        c.wait()

    parts = [recv1[i] for i in range(n)]
    top = functools.reduce(jnp.maximum, parts)
    tot = functools.reduce(jnp.add, [jnp.exp2(x - top) for x in parts])
    full = top + jnp.log(tot) * LOG2E
    for j in range(draft):
        lcol[pl.ds(j, seqs, stride=draft), :] = column(full[j:j + 1, :])[0:seqs, :]

    def excess(i, carry):
        r = pl.ds(pl.multiple_of(i * group, group), group)
        lr = lcol[r, :]
        acc = jnp.zeros((group, LANES), F32)
        for v in range(vtiles):
            size = min(LANES, vocab - v * LANES)
            e = jnp.maximum(jnp.exp2(scaled(r, v) - lr)[:, :size] - q_ref[r, v * LANES:v * LANES + size], 0.0)
            q_ref[r, v * LANES:v * LANES + size] = e
            acc = acc + (e if size == LANES else jnp.pad(e, ((0, 0), (0, LANES - size))))
        ta[r, :] = acc
        return carry

    lax.fori_loop(0, rows // group, excess, 0)

    for j in range(draft):
        part = jnp.sum(jnp.transpose(jnp.concatenate([rows_of(ta, j), rows_of(ta, j)], axis=0)),
                       axis=0, keepdims=True)
        tok = own[j:j + 1, :]
        owned = (tok >= 0) & (tok < vocab)
        ratio = jnp.minimum(1.0, jnp.exp2(picked[j] - full[j:j + 1, :])
                            / jnp.where(owned, pltpu.roll(picked[j], half, 1), 1.0))
        ratio = jnp.where(owned, ratio, 0.0)
        both = jnp.where(lane[0:1] < half, part, pltpu.roll(ratio, half, 1))
        send2[j:j + 1, :] = both
        recv2[me, j:j + 1, :] = both

    second = exchange(send2, recv2, s2_sem, r2_sem)
    for c in second:
        c.start()
    for c in second:
        c.wait()
    summed = functools.reduce(jnp.add, [recv2[i] for i in range(n)])
    stat[0:4, :] = summed
    stat[4:8, :] = pltpu.roll(full * LN2, half, 1)
    for j in range(draft):
        icol[pl.ds(j, seqs, stride=draft), :] = column(1.0 / summed[j:j + 1, :])[0:seqs, :]


def write_kernel(dims, exc_ref, icol_ref, stat_ref,
                 out_ref, accept_hbm, norm_hbm, bonus_hbm, accept_ref, norm_ref, bonus_ref, stage, sem, small_sem):
    seqs, draft, depth, vocab = dims
    rows = seqs * draft
    vtiles = pl.cdiv(vocab, LANES)
    group = 16
    per = group // draft

    norm_ref[...] = stat_ref[0:draft, 0:seqs]
    accept_ref[...] = pltpu.roll(stat_ref[0:draft, :], seqs, 1)[:, 0:seqs]
    bonus_ref[...] = stat_ref[4:5, 0:seqs]
    small = [pltpu.make_async_copy(a, b, small_sem.at[i]) for i, (a, b) in enumerate(
        [(accept_ref, accept_hbm), (norm_ref, norm_hbm), (bonus_ref, bonus_hbm)])]

    def copy(b, row):
        return pltpu.make_async_copy(stage.at[pl.ds(row, draft), :], out_ref.at[b], sem.at[b])

    @pl.loop(0, rows // group)
    def _(i):
        base = pl.multiple_of(i * group, group)
        r = pl.ds(base, group)
        inv = icol_ref[r, :]
        for v in range(vtiles):
            size = min(LANES, vocab - v * LANES)
            stage[r, v * LANES:v * LANES + size] = exc_ref[r, v * LANES:v * LANES + size] * inv[:, :size]
        for b in range(per):
            copy(i * per + b, base + b * draft).start(priority=b % 2)

    for c in small:
        c.start()
    for b in range(seqs):
        copy(b, b * draft).wait()
    for c in small:
        c.wait()


def solution(mesh):
    n = mesh.shape["tp"]

    def local_step(hidden, norm_gain, w_head, draft_probs, draft_tokens, temperature):
        seqs, draft, vocab = draft_probs.shape
        depth = w_head.shape[0]
        dims = (seqs, draft, depth, vocab)
        rows = seqs * draft
        total = rows + seqs
        zwide = stream_blocks(vocab) * BLOCK
        ttail = vocab - zwide
        twide = pl.cdiv(ttail, LANES) * LANES
        vmem = pl.BlockSpec(memory_space=pltpu.VMEM)
        hbm = pl.BlockSpec(memory_space=pl.ANY)

        def held(xs):
            return [pltpu.with_memory_space_constraint(x, pltpu.VMEM) for x in xs]

        streamed = pl.pallas_call(
            functools.partial(stream_kernel, dims),
            out_shape=(pltpu.VMEM((rows, zwide), F32),
                       pltpu.VMEM((total, depth), BF16), pltpu.VMEM((ttail, depth), BF16),
                       pltpu.VMEM((total, LANES), F32), pltpu.VMEM((total, LANES), F32),
                       pltpu.VMEM((rows, LANES), F32), pltpu.VMEM((total, LANES), F32),
                       pltpu.VMEM((draft, LANES), jnp.int32)),
            in_specs=[hbm] * 5,
            out_specs=(vmem,) * 8,
            scratch_shapes=[
                pltpu.VMEM((draft + 1, seqs, depth), BF16),
                pltpu.VMEM((4, rows, LANES), F32),
                pltpu.VMEM((SLOTS, BLOCK, depth), BF16),
                pltpu.VMEM((8, LANES), F32),
                pltpu.VMEM((1, depth), F32),
                pltpu.VMEM((1, seqs), F32),
                pltpu.VMEM((draft, seqs), jnp.int32),
                pltpu.VMEM((draft + 1, seqs, LANES), F32),
                pltpu.SemaphoreType.DMA((draft + 1,)),
                pltpu.SemaphoreType.DMA((SLOTS,)),
                pltpu.SemaphoreType.DMA,
                pltpu.SemaphoreType.DMA((3,)),
                pltpu.SemaphoreType.DMA((2,)),
            ],
            compiler_params=pltpu.CompilerParams(vmem_limit_bytes=30 * 1024 * 1024),
            name="verify_stream",
        )(*[pltpu.with_memory_space_constraint(x, pltpu.HBM) for x in (
            jnp.transpose(hidden, (1, 0, 2)), norm_gain.reshape(1, depth), w_head.T,
            temperature.reshape(1, seqs), draft_tokens.T)])

        shared = pl.pallas_call(
            functools.partial(exchange_kernel, dims, n),
            out_shape=(pltpu.VMEM((rows, vocab), F32), pltpu.VMEM((rows, LANES), F32),
                       pltpu.VMEM((8, LANES), F32)),
            in_specs=[hbm] + [vmem] * 8,
            out_specs=(vmem,) * 3,
            scratch_shapes=[
                pltpu.VMEM((total, twide), F32),
                pltpu.VMEM((rows, LANES), F32),
                pltpu.VMEM((total, LANES), F32),
                pltpu.VMEM((total, LANES), F32),
                pltpu.VMEM((rows, LANES), F32),
                pltpu.VMEM((rows, LANES), F32),
                pltpu.VMEM((4, LANES), F32),
                pltpu.VMEM((n, 4, LANES), F32),
                pltpu.VMEM((4, LANES), F32),
                pltpu.VMEM((n, 4, LANES), F32),
                pltpu.SemaphoreType.DMA((seqs,)),
                pltpu.SemaphoreType.DMA((n,)),
                pltpu.SemaphoreType.DMA((n,)),
                pltpu.SemaphoreType.DMA((n,)),
                pltpu.SemaphoreType.DMA((n,)),
            ],
            compiler_params=pltpu.CompilerParams(
                collective_id=0, has_side_effects=True, vmem_limit_bytes=6 * 1024 * 1024),
            name="verify_exchange",
        )(pltpu.with_memory_space_constraint(draft_probs, pltpu.HBM), *held(streamed))

        residual, accept, norm_sum, bonus = pl.pallas_call(
            functools.partial(write_kernel, dims),
            out_shape=(jax.ShapeDtypeStruct((seqs, draft, vocab), F32),
                       jax.ShapeDtypeStruct((draft, seqs), F32), jax.ShapeDtypeStruct((draft, seqs), F32),
                       jax.ShapeDtypeStruct((1, seqs), F32)),
            in_specs=[vmem] * 3,
            out_specs=(hbm, hbm, hbm, hbm),
            scratch_shapes=[pltpu.VMEM((draft, seqs), F32), pltpu.VMEM((draft, seqs), F32), pltpu.VMEM((1, seqs), F32),
                            pltpu.VMEM((rows, vocab), F32), pltpu.SemaphoreType.DMA((seqs,)),
                            pltpu.SemaphoreType.DMA((3,))],
            compiler_params=pltpu.CompilerParams(vmem_limit_bytes=10 * 1024 * 1024),
            name="verify_write",
        )(*held(shared))

        return accept.T, norm_sum.T, residual, bonus.reshape(seqs)

    return jax.shard_map(
        local_step,
        mesh=mesh,
        in_specs=(P('dp', None, None), P(), P(None, 'tp'), P('dp', None, 'tp'), P('dp', None), P('dp')),
        out_specs=(P('dp', None), P('dp', None), P('dp', None, 'tp'), P('dp')),
        check_vma=False,
    )
```

```python
import functools

import jax
import jax.numpy as jnp
from jax import lax
from jax.experimental import pallas as pl
from jax.experimental.pallas import tpu as pltpu
from jax.sharding import PartitionSpec as P

MESH = pl.DeviceIdType.MESH
F32 = jnp.float32
BF16 = jnp.bfloat16
LOG2E = 1.4426950408889634
LN2 = 0.6931471805599453
NEG = -1e30
LANES = 128
TILE = 256
BLOCK = 2 * TILE
SLOTS = 6
PIECE = 64


def stream_blocks(vocab):
    return 2 * (vocab // (2 * BLOCK))


def column(row):
    return jnp.transpose(jnp.broadcast_to(row, (LANES, LANES)))


def stream_kernel(dims, hid_hbm, gain_hbm, wt_ref, temp_hbm, tok_hbm,
                  zs, xb, wtail, mx, sm, tokc, invc, own,
                  hid, xs, ring, row, gain_ref, temp_ref, tok_ref, rr, hid_sem, w_sem, t_sem, c_sem, f_sem):
    seqs, draft, depth, vocab = dims
    rows = seqs * draft
    total = rows + seqs
    ktiles = depth // TILE
    nblocks = stream_blocks(vocab)
    tail = vocab - nblocks * BLOCK
    pieces = total // PIECE
    chunks = depth // LANES

    def w_copy(block):
        slot = lax.rem(block, SLOTS)
        return pltpu.make_async_copy(
            wt_ref.at[pl.ds(pl.multiple_of(block * BLOCK, BLOCK), BLOCK), :], ring.at[slot], w_sem.at[slot])

    tail_copy = pltpu.make_async_copy(wt_ref.at[pl.ds(nblocks * BLOCK, tail), :], wtail, t_sem)
    hid_copies = [pltpu.make_async_copy(hid_hbm.at[j], hid.at[j], hid_sem.at[j]) for j in range(draft + 1)]
    small = [pltpu.make_async_copy(a, b, c_sem.at[i]) for i, (a, b) in enumerate(
        [(temp_hbm, temp_ref), (tok_hbm, tok_ref), (gain_hbm, gain_ref)])]
    for c in small + hid_copies:
        c.start()
    fold = depth // 2
    first_copies = [pltpu.make_async_copy(
        wt_ref.at[pl.ds(0, BLOCK), pl.ds(i * fold, fold)], ring.at[0, :, pl.ds(i * fold, fold)], f_sem.at[i])
        for i in range(2)]
    for c in first_copies:
        c.start(priority=1)
    for i in range(1, SLOTS):
        w_copy(i).start(priority=1)

    mx[...] = jnp.full(mx.shape, NEG, F32)
    sm[...] = jnp.ones(sm.shape, F32)
    row[...] = jnp.ones(row.shape, F32)
    own[...] = jnp.zeros(own.shape, jnp.int32)
    for c in small:
        c.wait()
    row[0:1, 0:seqs] = temp_ref[...]
    own[:, 0:seqs] = tok_ref[...] - lax.axis_index("tp") * vocab
    row[1:1 + draft, 0:seqs] = own[:, 0:seqs].astype(F32)
    inv = LOG2E / column(row[0:1, :])[0:seqs, :]
    for j in range(draft):
        invc[pl.ds(j, seqs, stride=draft), :] = inv
        tokc[pl.ds(j, seqs, stride=draft), :] = column(row[1 + j:2 + j, :])[0:seqs, :]
    invc[pl.ds(rows, seqs), :] = inv

    for j in range(draft + 1):
        hid_copies[j].wait()

        def squares(c, acc, j=j):
            for u in range(16):
                h = hid[j, :, pl.ds(pl.multiple_of((c * 16 + u) * LANES, LANES), LANES)].astype(F32)
                acc = acc + h * h
            return acc

        s = lax.fori_loop(0, chunks // 16, squares, jnp.zeros((seqs, LANES), F32))
        r = lax.rsqrt(jnp.sum(s, axis=-1, keepdims=True) * (1.0 / depth) + 1e-5)
        rr[j] = jnp.broadcast_to(r, (seqs, LANES))

    def normalise(k):
        for u in range(2):
            lanes = slice((k * 2 + u) * LANES, (k * 2 + u + 1) * LANES)
            slab = (k * 2 + u) % 4
            g = gain_ref[:, lanes]
            for j in range(draft + 1):
                x = hid[j, :, lanes].astype(F32) * rr[j] * g
                if j < draft:
                    xs[slab, pl.ds(j, seqs, stride=draft), :] = x
                else:
                    xb[pl.ds(rows, seqs), lanes] = x.astype(BF16)
            xb[pl.ds(0, rows), lanes] = xs[slab].astype(BF16)

    normalise(0)

    def stream(*accs):
        acc = [[accs[(par * 2 + q) * pieces:(par * 2 + q + 1) * pieces] for q in range(2)] for par in range(2)]

        def push(slot, k, q):
            pltpu.matmul_push_rhs(ring[slot, q * TILE:(q + 1) * TILE, k * TILE:(k + 1) * TILE],
                                  staging_register=k % 2, mxu_index=q, transpose=True)

        def process(par, block, which):
            for p in which:
                z = [pltpu.matmul_pop(acc[par][q][p]) for q in range(2)]
                r = pl.ds(p * PIECE, PIECE)
                inv = invc[r, :]
                s = [z[g // 2][:, (g % 2) * LANES:(g % 2 + 1) * LANES] * inv for g in range(4)]
                if (p + 1) * PIECE <= rows:
                    for g in range(4):
                        zs[r, pl.ds(pl.multiple_of(block * BLOCK + g * LANES, LANES), LANES)] = s[g]
                m_old = mx[r, :]
                m_new = jnp.maximum(jnp.maximum(m_old, jnp.maximum(s[0], s[1])), jnp.maximum(s[2], s[3]))
                e = sm[r, :] * jnp.exp2(m_old - m_new)
                e = e + ((jnp.exp2(s[0] - m_new) + jnp.exp2(s[1] - m_new))
                         + (jnp.exp2(s[2] - m_new) + jnp.exp2(s[3] - m_new)))
                mx[r, :] = m_new
                sm[r, :] = e

        def half(block, par, first=False, last=False, fetch=False):
            slot = lax.rem(block, SLOTS)
            after = lax.rem(block + 1, SLOTS)
            for k in range(ktiles):
                if first and k == ktiles // 2 - 1:
                    first_copies[1].wait()
                if k == ktiles - 1:
                    if not last:
                        w_copy(block + 1).wait()
                    if fetch:
                        w_copy(block - 1 + SLOTS).start(priority=1)
                if first and k + 1 < ktiles:
                    normalise(k + 1)
                for q in range(2):
                    if k + 1 < ktiles:
                        push(slot, k + 1, q)
                    elif not last:
                        push(after, 0, q)
                for p in range(pieces):
                    x = xb[p * PIECE:(p + 1) * PIECE, k * TILE:(k + 1) * TILE]
                    for q in range(2):
                        pltpu.matmul_acc_lhs(acc[par][q][p], x, load_staged_rhs=(k % 2) if p == 0 else None)
                if k % 2 == 1 and k // 2 < pieces and not first:
                    process(1 - par, block - 1, [k // 2])

        for c in first_copies[:1]:
            c.wait()
        for q in range(2):
            push(0, 0, q)
        half(0, 0, first=True)
        steady = (nblocks - SLOTS) // 2

        @pl.loop(0, steady)
        def _(trip):
            half(trip * 2 + 1, 1, fetch=True)
            half(trip * 2 + 2, 0, fetch=True)

        tail_copy.start(priority=1)

        @pl.loop(steady, (nblocks - 2) // 2)
        def _(trip):
            half(trip * 2 + 1, 1)
            half(trip * 2 + 2, 0)

        half(nblocks - 1, 1, last=True)
        process(1, nblocks - 1, range(pieces))

    pl.run_scoped(stream, *[pltpu.ACC(q)((PIECE, TILE), F32)
                            for _ in range(2) for q in range(2) for _ in range(pieces)])
    tail_copy.wait()


def exchange_kernel(dims, n, q_hbm, zs_ref, xb_ref, wtail_ref, mx_ref, sm_ref, tokc_ref, invc_ref, own,
                    q_ref, icol, stat,
                    zt, lcol, pt, mx, sm, ta, tb, send1, recv1, send2, recv2, q_sem, s1_sem, r1_sem, s2_sem, r2_sem):
    seqs, draft, depth, vocab = dims
    rows = seqs * draft
    total = rows + seqs
    me = lax.axis_index("tp")
    first_tail = stream_blocks(vocab) * BLOCK
    tail = vocab - first_tail
    vtiles = pl.cdiv(vocab, LANES)
    ttiles = pl.cdiv(tail, LANES)
    lane = lax.broadcasted_iota(jnp.int32, (8, LANES), 1)
    half = seqs

    barrier = pltpu.get_barrier_semaphore()
    for d in range(1, n):
        pl.semaphore_signal(barrier, inc=1, device_id={"tp": lax.rem(me + d, n)}, device_id_type=MESH)

    q_copies = [pltpu.make_async_copy(q_hbm.at[b], q_ref.at[pl.ds(b * draft, draft), :], q_sem.at[b])
                for b in range(seqs)]
    for c in q_copies:
        c.start(priority=1)

    zt[:, :tail] = lax.dot_general(xb_ref[...], wtail_ref[...], (((1,), (1,)), ((), ())),
                                   preferred_element_type=F32)
    step = 32

    def finish(i, is_draft):
        r = pl.ds(pl.multiple_of(i * step, step), step)
        inv = invc_ref[r, :]
        s = []
        for g in range(ttiles):
            v = zt[r, g * LANES:(g + 1) * LANES] * inv
            if (g + 1) * LANES > tail:
                v = jnp.where(jnp.broadcast_to((lane + g * LANES < tail)[0:1], (step, LANES)), v, NEG)
            s.append(v)
        if is_draft:
            for g in range(ttiles):
                zt[r, g * LANES:(g + 1) * LANES] = s[g]
        m_old = mx_ref[r, :]
        m_new = functools.reduce(jnp.maximum, s, m_old)
        e = sm_ref[r, :] * jnp.exp2(m_old - m_new)
        for v in s:
            e = e + jnp.exp2(v - m_new)
        mx[r, :] = m_new
        sm[r, :] = e

    @pl.loop(0, rows // step)
    def _(i):
        finish(i, True)

    @pl.loop(rows // step, total // step)
    def _(i):
        finish(i, False)

    def rows_of(ref, j):
        return ref[pl.ds(j, seqs, stride=draft), :]

    local = []
    for j in range(draft):
        mt = jnp.transpose(jnp.concatenate([rows_of(mx, j), mx[pl.ds(rows, seqs), :]], axis=0))
        st = jnp.transpose(jnp.concatenate([rows_of(sm, j), sm[pl.ds(rows, seqs), :]], axis=0))
        top = jnp.max(mt, axis=0, keepdims=True)
        tot = jnp.sum(st * jnp.exp2(mt - top), axis=0, keepdims=True)
        lse = top + jnp.log(tot) * LOG2E
        send1[j:j + 1, :] = lse
        recv1[me, j:j + 1, :] = lse
        local.append(lse)

    pl.semaphore_wait(barrier, n - 1)

    def exchange(send, recv, s_sem, r_sem):
        return [pltpu.make_async_remote_copy(
            src_ref=send, dst_ref=recv.at[me], send_sem=s_sem.at[d], recv_sem=r_sem.at[d],
            device_id={"tp": lax.rem(me + d, n)}, device_id_type=MESH) for d in range(1, n)]

    first = exchange(send1, recv1, s1_sem, r1_sem)
    for c in first:
        c.start()

    for j in range(draft):
        lcol[pl.ds(j, seqs, stride=draft), :] = column(local[j])[0:seqs, :]
    for c in q_copies:
        c.wait()

    group = 32

    def scaled(r, v):
        off = v * LANES - first_tail
        return zs_ref[r, v * LANES:(v + 1) * LANES] if off < 0 else zt[r, off:off + LANES]

    def gather(i, carry):
        r = pl.ds(pl.multiple_of(i * group, group), group)
        tokr = tokc_ref[r, :]
        lr = lcol[r, :]
        acc_s = jnp.zeros((group, LANES), F32)
        acc_q = jnp.zeros((group, LANES), F32)
        for v in range(vtiles):
            size = min(LANES, vocab - v * LANES)
            hit = tokr == (lane + v * LANES).astype(F32)[0:1]
            sv = scaled(r, v)
            pt[r, v * LANES:(v + 1) * LANES] = jnp.exp2(sv - lr)
            acc_s = acc_s + jnp.where(hit, sv, 0.0)
            if size == LANES:
                acc_q = acc_q + jnp.where(hit, q_ref[r, v * LANES:(v + 1) * LANES], 0.0)
            else:
                part = jnp.where(hit[:, :size], q_ref[r, v * LANES:v * LANES + size], 0.0)
                acc_q = acc_q + jnp.pad(part, ((0, 0), (0, LANES - size)))
        ta[r, :] = acc_s
        tb[r, :] = acc_q
        return carry

    lax.fori_loop(0, rows // group, gather, 0)
    picked = [jnp.sum(jnp.transpose(jnp.concatenate([rows_of(ta, j), rows_of(tb, j)], axis=0)),
                      axis=0, keepdims=True) for j in range(draft)]

    for c in first:
        c.wait()

    parts = [recv1[i] for i in range(n)]
    top = functools.reduce(jnp.maximum, parts)
    tot = functools.reduce(jnp.add, [jnp.exp2(x - top) for x in parts])
    full = top + jnp.log(tot) * LOG2E
    for j in range(draft):
        lcol[pl.ds(j, seqs, stride=draft), :] = column(jnp.exp2(local[j] - full[j:j + 1, :]))[0:seqs, :]

    def excess(i, carry):
        r = pl.ds(pl.multiple_of(i * group, group), group)
        lr = lcol[r, :]
        acc = jnp.zeros((group, LANES), F32)
        for v in range(vtiles):
            size = min(LANES, vocab - v * LANES)
            e = jnp.maximum((pt[r, v * LANES:(v + 1) * LANES] * lr)[:, :size] - q_ref[r, v * LANES:v * LANES + size], 0.0)
            q_ref[r, v * LANES:v * LANES + size] = e
            acc = acc + (e if size == LANES else jnp.pad(e, ((0, 0), (0, LANES - size))))
        ta[r, :] = acc
        return carry

    lax.fori_loop(0, rows // group, excess, 0)

    for j in range(draft):
        part = jnp.sum(jnp.transpose(jnp.concatenate([rows_of(ta, j), rows_of(ta, j)], axis=0)),
                       axis=0, keepdims=True)
        tok = own[j:j + 1, :]
        owned = (tok >= 0) & (tok < vocab)
        ratio = jnp.minimum(1.0, jnp.exp2(picked[j] - full[j:j + 1, :])
                            / jnp.where(owned, pltpu.roll(picked[j], half, 1), 1.0))
        ratio = jnp.where(owned, ratio, 0.0)
        both = jnp.where(lane[0:1] < half, part, pltpu.roll(ratio, half, 1))
        send2[j:j + 1, :] = both
        recv2[me, j:j + 1, :] = both

    second = exchange(send2, recv2, s2_sem, r2_sem)
    for c in second:
        c.start()
    for c in second:
        c.wait()
    summed = functools.reduce(jnp.add, [recv2[i] for i in range(n)])
    stat[0:4, :] = summed
    stat[4:8, :] = pltpu.roll(full * LN2, half, 1)
    for j in range(draft):
        icol[pl.ds(j, seqs, stride=draft), :] = column(1.0 / summed[j:j + 1, :])[0:seqs, :]


def write_kernel(dims, exc_ref, icol_ref, stat_ref,
                 out_ref, accept_hbm, norm_hbm, bonus_hbm, accept_ref, norm_ref, bonus_ref, stage, sem, small_sem):
    seqs, draft, depth, vocab = dims
    rows = seqs * draft
    vtiles = pl.cdiv(vocab, LANES)
    group = 16
    per = group // draft

    norm_ref[...] = stat_ref[0:draft, 0:seqs]
    accept_ref[...] = pltpu.roll(stat_ref[0:draft, :], seqs, 1)[:, 0:seqs]
    bonus_ref[...] = stat_ref[4:5, 0:seqs]
    small = [pltpu.make_async_copy(a, b, small_sem.at[i]) for i, (a, b) in enumerate(
        [(accept_ref, accept_hbm), (norm_ref, norm_hbm), (bonus_ref, bonus_hbm)])]

    def copy(b, row):
        return pltpu.make_async_copy(stage.at[pl.ds(row, draft), :], out_ref.at[b], sem.at[b])

    @pl.loop(0, rows // group)
    def _(i):
        base = pl.multiple_of(i * group, group)
        r = pl.ds(base, group)
        inv = icol_ref[r, :]
        for v in range(vtiles):
            size = min(LANES, vocab - v * LANES)
            stage[r, v * LANES:v * LANES + size] = exc_ref[r, v * LANES:v * LANES + size] * inv[:, :size]
        for b in range(per):
            copy(i * per + b, base + b * draft).start(priority=b % 2)

    for c in small:
        c.start()
    for b in range(seqs):
        copy(b, b * draft).wait()
    for c in small:
        c.wait()


def solution(mesh):
    n = mesh.shape["tp"]

    def local_step(hidden, norm_gain, w_head, draft_probs, draft_tokens, temperature):
        seqs, draft, vocab = draft_probs.shape
        depth = w_head.shape[0]
        dims = (seqs, draft, depth, vocab)
        rows = seqs * draft
        total = rows + seqs
        zwide = stream_blocks(vocab) * BLOCK
        ttail = vocab - zwide
        twide = pl.cdiv(ttail, LANES) * LANES
        vmem = pl.BlockSpec(memory_space=pltpu.VMEM)
        hbm = pl.BlockSpec(memory_space=pl.ANY)

        def held(xs):
            return [pltpu.with_memory_space_constraint(x, pltpu.VMEM) for x in xs]

        streamed = pl.pallas_call(
            functools.partial(stream_kernel, dims),
            out_shape=(pltpu.VMEM((rows, zwide), F32),
                       pltpu.VMEM((total, depth), BF16), pltpu.VMEM((ttail, depth), BF16),
                       pltpu.VMEM((total, LANES), F32), pltpu.VMEM((total, LANES), F32),
                       pltpu.VMEM((rows, LANES), F32), pltpu.VMEM((total, LANES), F32),
                       pltpu.VMEM((draft, LANES), jnp.int32)),
            in_specs=[hbm] * 5,
            out_specs=(vmem,) * 8,
            scratch_shapes=[
                pltpu.VMEM((draft + 1, seqs, depth), BF16),
                pltpu.VMEM((4, rows, LANES), F32),
                pltpu.VMEM((SLOTS, BLOCK, depth), BF16),
                pltpu.VMEM((8, LANES), F32),
                pltpu.VMEM((1, depth), F32),
                pltpu.VMEM((1, seqs), F32),
                pltpu.VMEM((draft, seqs), jnp.int32),
                pltpu.VMEM((draft + 1, seqs, LANES), F32),
                pltpu.SemaphoreType.DMA((draft + 1,)),
                pltpu.SemaphoreType.DMA((SLOTS,)),
                pltpu.SemaphoreType.DMA,
                pltpu.SemaphoreType.DMA((3,)),
                pltpu.SemaphoreType.DMA((2,)),
            ],
            compiler_params=pltpu.CompilerParams(vmem_limit_bytes=30 * 1024 * 1024),
            name="verify_stream",
        )(*[pltpu.with_memory_space_constraint(x, pltpu.HBM) for x in (
            jnp.transpose(hidden, (1, 0, 2)), norm_gain.reshape(1, depth), w_head.T,
            temperature.reshape(1, seqs), draft_tokens.T)])

        shared = pl.pallas_call(
            functools.partial(exchange_kernel, dims, n),
            out_shape=(pltpu.VMEM((rows, vocab), F32), pltpu.VMEM((rows, LANES), F32),
                       pltpu.VMEM((8, LANES), F32)),
            in_specs=[hbm] + [vmem] * 8,
            out_specs=(vmem,) * 3,
            scratch_shapes=[
                pltpu.VMEM((total, twide), F32),
                pltpu.VMEM((rows, LANES), F32),
                pltpu.VMEM((rows, zwide + twide), F32),
                pltpu.VMEM((total, LANES), F32),
                pltpu.VMEM((total, LANES), F32),
                pltpu.VMEM((rows, LANES), F32),
                pltpu.VMEM((rows, LANES), F32),
                pltpu.VMEM((4, LANES), F32),
                pltpu.VMEM((n, 4, LANES), F32),
                pltpu.VMEM((4, LANES), F32),
                pltpu.VMEM((n, 4, LANES), F32),
                pltpu.SemaphoreType.DMA((seqs,)),
                pltpu.SemaphoreType.DMA((n,)),
                pltpu.SemaphoreType.DMA((n,)),
                pltpu.SemaphoreType.DMA((n,)),
                pltpu.SemaphoreType.DMA((n,)),
            ],
            compiler_params=pltpu.CompilerParams(
                collective_id=0, has_side_effects=True, vmem_limit_bytes=15 * 1024 * 1024),
            name="verify_exchange",
        )(pltpu.with_memory_space_constraint(draft_probs, pltpu.HBM), *held(streamed))

        residual, accept, norm_sum, bonus = pl.pallas_call(
            functools.partial(write_kernel, dims),
            out_shape=(jax.ShapeDtypeStruct((seqs, draft, vocab), F32),
                       jax.ShapeDtypeStruct((draft, seqs), F32), jax.ShapeDtypeStruct((draft, seqs), F32),
                       jax.ShapeDtypeStruct((1, seqs), F32)),
            in_specs=[vmem] * 3,
            out_specs=(hbm, hbm, hbm, hbm),
            scratch_shapes=[pltpu.VMEM((draft, seqs), F32), pltpu.VMEM((draft, seqs), F32), pltpu.VMEM((1, seqs), F32),
                            pltpu.VMEM((rows, vocab), F32), pltpu.SemaphoreType.DMA((seqs,)),
                            pltpu.SemaphoreType.DMA((3,))],
            compiler_params=pltpu.CompilerParams(vmem_limit_bytes=10 * 1024 * 1024),
            name="verify_write",
        )(*held(shared))

        return accept.T, norm_sum.T, residual, bonus.reshape(seqs)

    return jax.shard_map(
        local_step,
        mesh=mesh,
        in_specs=(P('dp', None, None), P(), P(None, 'tp'), P('dp', None, 'tp'), P('dp', None), P('dp')),
        out_specs=(P('dp', None), P('dp', None), P('dp', None, 'tp'), P('dp')),
        check_vma=False,
    )
```
